32 devices in a mesh: dp: 8 (over z, x), mp: 4 (over y, core).
Axes of the slice: x: 2, y: 2, z: 4, core: 2. Of those that a mesh axis runs over, the one named last changes fastest.
Arguments:
- tokens: bfloat16 [8192, 2048], P('dp', 'mp'), may hold values from -6 to 6
- norm_gain: bfloat16 [2048], replicated, may hold values from 0.099609375 to 1.8984375
- wi_gate: bfloat16 [2048, 5120], P(None, 'mp'), may hold values from -0.125 to 0.125
- wi_linear: bfloat16 [2048, 5120], P(None, 'mp'), may hold values from -0.125 to 0.125
- wo_out: bfloat16 [5120, 2048], P('mp'), may hold values from -0.078125 to 0.078125
- task_table: float32 [8, 64], replicated, may hold values from -5 to 5
- layer_table: float32 [24, 64], replicated, may hold values from -5 to 5
- task_ids: int32 [64], P('dp'), may hold values from 0 to 7
- layer_index: int32 [1], replicated, may hold values from 0 to 23
- hyper_in: bfloat16 [128, 1024], P(None, 'mp'), may hold values from -0.5 to 0.5
- gen_down: bfloat16 [1024, 131072], P(None, ('mp', 'dp')), may hold values from -0.0078125 to 0.0078125
- gen_up: bfloat16 [1024, 131072], P(None, ('mp', 'dp')), may hold values from -0.046875 to 0.046875
Outputs:
- mixed: bfloat16 [8192, 2048], P('dp', 'mp')
The draws below stay inside these ranges and needn't reach their ends.
All inputs are finite; a program needn't handle non-finite values.
Results may differ from the reference program's by a relative error of at most 0.019.
Values may be sent and summed in bfloat16 or wider, within the bound.
A program may use at most 128 MiB of HBM per device.

```python
import jax
import jax.numpy as jnp
from jax import lax

D = 2048
FF = 5120
R = 64
HID = 1024
EMB = 64
TASKS = 8
LAYERS = 24
SEQ = 128
SEQS = 64
TOKENS = 8192
N_MP = 4


def touch_ends(drawn, own_key, smallest, top_value):
    shape = drawn.shape
    place = [jax.random.randint(jax.random.fold_in(own_key, axis), (), 0, shape[axis]) for axis in range(len(shape))]
    drawn = drawn.at[tuple(place)].set(smallest)
    longest = shape.index(max(shape))
    place[longest] = (place[longest] + 1) % shape[longest]
    return drawn.at[tuple(place)].set(top_value)


def steps_of(rng, dims, pieces, low, top_value):
    factor_of, own = 1.0, jax.random.fold_in(rng, 6)
    for dim, shards_of in pieces:
        draws = jnp.exp(jax.random.uniform(jax.random.fold_in(own, dim), (shards_of,), jnp.float32, low / len(pieces), top_value / len(pieces)))
        factor_of = factor_of * jnp.repeat(draws, dims[dim] // shards_of).reshape([-1 if axis == dim else 1 for axis in range(len(dims))])
    return factor_of


def noise(stream_key, dims, scale, reach, shards=(), kind=jnp.bfloat16):
    entries = jax.random.normal(stream_key, dims, jnp.float32) * scale
    if len(shards) > 0:
        entries = steps_of(stream_key, dims, shards, -0.22, 0.18) * entries
    return jnp.clip(entries, min=-reach, max=reach).astype(kind)


def setup_inputs(seed: int = 0) -> dict:
    seeds = jax.random.split(jax.random.key(seed), 13)
    tokens = noise(seeds[0], (TOKENS, D), 1.0, 6.0, ((0, 8), (1, 4)))
    norm_gain = jnp.clip(1.0 + 0.18 * jax.random.normal(seeds[1], (D,), jnp.float32), 0.099609375, 1.8984375).astype(jnp.bfloat16)
    wi_gate = noise(seeds[2], (D, FF), D ** -0.5, 0.125, ((1, 4),))
    wi_linear = noise(seeds[3], (D, FF), D ** -0.5, 0.125, ((1, 4),))
    wo_out = noise(seeds[4], (FF, D), FF ** -0.5, 0.078125, ((0, 4),))
    task_table = noise(seeds[5], (TASKS, EMB), 1.0, 5.0, (), jnp.float32)
    layer_table = noise(seeds[6], (LAYERS, EMB), 1.0, 5.0, (), jnp.float32)
    task_ids = touch_ends(jax.random.randint(seeds[7], (SEQS,), 0, TASKS), jax.random.fold_in(seeds[7], 1), 0, TASKS - 1).astype(jnp.int32)
    layer_index = jax.random.randint(seeds[8], (1,), 0, LAYERS).astype(jnp.int32)
    hyper_in = noise(seeds[9], (2 * EMB, HID), (2 * EMB) ** -0.5, 0.5, ((1, 4),))
    gen_down = noise(seeds[10], (HID, D * R), (HID * D // 4) ** -0.5, 0.0078125, ((1, 32),))
    gen_up = noise(seeds[11], (HID, D * R), (HID * R // 4) ** -0.5, 0.046875, ((1, 32),))
    return {"tokens": tokens, "norm_gain": norm_gain, "wi_gate": wi_gate, "wi_linear": wi_linear, "wo_out": wo_out, "task_table": task_table, "layer_table": layer_table, "task_ids": task_ids, "layer_index": layer_index, "hyper_in": hyper_in, "gen_down": gen_down, "gen_up": gen_up}


def reference(tokens, norm_gain, wi_gate, wi_linear, wo_out, task_table, layer_table, task_ids, layer_index, hyper_in, gen_down, gen_up):
    layer_row = jnp.take(layer_table, layer_index, axis=0)
    embed = jnp.concatenate([task_table, jnp.broadcast_to(layer_row, (TASKS, EMB))], axis=1).astype(jnp.bfloat16)
    hidden = jnp.maximum(jnp.dot(embed, hyper_in, preferred_element_type=jnp.float32), 0.0).astype(jnp.bfloat16)
    down_all = jnp.dot(hidden, gen_down, preferred_element_type=jnp.float32).astype(jnp.bfloat16)
    up_all = jnp.dot(hidden, gen_up, preferred_element_type=jnp.float32).astype(jnp.bfloat16)
    wide = tokens.astype(jnp.float32)
    scale = jax.lax.rsqrt(lax.optimization_barrier(jnp.mean(wide * wide, axis=-1, keepdims=True)) + 1e-06)
    normed = (wide * scale * norm_gain.astype(jnp.float32)).astype(jnp.bfloat16)
    gate = jnp.dot(normed, wi_gate, preferred_element_type=jnp.float32)
    linear = jnp.dot(normed, wi_linear, preferred_element_type=jnp.float32)
    act = (jax.nn.gelu(gate, approximate=True) * linear).astype(jnp.bfloat16)
    group = FF // N_MP

    def add_group(total, index):
        start = (index * group).astype(jnp.int32)
        cols = lax.dynamic_slice_in_dim(act, start, group, 1)
        rows = lax.dynamic_slice_in_dim(wo_out, start, group, 0)
        piece = jnp.dot(cols, rows, preferred_element_type=jnp.float32).astype(jnp.bfloat16)
        piece = lax.optimization_barrier(piece)
        return (total + piece.astype(jnp.float32), None)
    summed, unused = lax.scan(add_group, jnp.zeros((TOKENS, D), jnp.float32), jnp.arange(N_MP, dtype=jnp.int32))
    ffout = summed.astype(jnp.bfloat16)
    seq_down = jnp.take(down_all, task_ids, axis=0).reshape(SEQS, D, R).astype(jnp.float32)
    seq_up = jnp.take(up_all, task_ids, axis=0).reshape(SEQS, D, R).astype(jnp.float32)
    blocks = ffout.astype(jnp.float32).reshape(SEQS, SEQ, D)
    squeezed = jnp.maximum(jnp.einsum('std,sdr->str', blocks, seq_down), 0.0).astype(jnp.bfloat16)
    expand = jnp.einsum('str,sdr->std', squeezed.astype(jnp.float32), seq_up).reshape(TOKENS, D)
    return (wide + ffout.astype(jnp.float32) + expand).astype(jnp.bfloat16)
```

```python
import functools

import jax
import jax.numpy as jnp
from jax import lax
from jax.experimental import pallas as pl
from jax.experimental.pallas import tpu as pltpu
from jax.sharding import PartitionSpec as P

F32, BF16 = jnp.float32, jnp.bfloat16
LANES = 128


def matmul(left, right):
    return jnp.dot(left, right, preferred_element_type=F32)


def kernel(
    n_dp, n_mp, rank,
    ids_ref, layer_at, gain_ref, task_ref, layer_ref, hyper_ref,
    tok, w_gate, w_lin, w_out, g_down, g_up,
    out,
    x_all, wg, wl, wo, gd, gu, normed, act, hid, made_all, down, up,
    part_mine, part_away, part_got, y_out, y_got, ff_all,
    sq_mine, sq_got, sq_chip, sq_far, result,
    load_sem, out_sem,
    ag_s, ag_r, pair_s, pair_r, fw_s, fw_r, hid_s, hid_r,
    gen_s, gen_r, pt_s, pt_r, y_s, y_r, sp_s, sp_r, sf_s, sf_r,
):
    dp, mp = lax.axis_index("dp"), lax.axis_index("mp")
    chips = n_mp // 2
    core, chip = lax.rem(mp, 2), lax.div(mp, 2)
    mate = chip * 2 + 1 - core
    rows_all, feat = tok.shape
    seqs = ids_ref.shape[0]
    seq = rows_all // seqs
    steps = part_mine.shape[0]
    rows = rows_all // steps
    tasks = task_ref.shape[0]
    model = feat * n_mp

    def remote(src, dst, send, recv, to_mp=None, to_dp=None):
        return pltpu.make_async_remote_copy(
            src_ref=src, dst_ref=dst, send_sem=send, recv_sem=recv,
            device_id={"dp": dp if to_dp is None else to_dp, "mp": mp if to_mp is None else to_mp},
            device_id_type=pl.DeviceIdType.MESH,
        )

    def far(off):
        return lax.rem(chip + off, chips)

    def src_chip(off):
        return lax.rem(chip + chips - off, chips)

    own_load = pltpu.make_async_copy(tok, x_all.at[mp], load_sem.at[0])
    loads = [
        pltpu.make_async_copy(src, dst, load_sem.at[i + 1])
        for i, (src, dst) in enumerate(
            [(g_down, gd), (g_up, gu), (w_gate, wg), (w_lin, wl), (w_out, wo)]
        )
    ]
    own_load.start()
    for load in loads:
        load.start()

    barrier = pltpu.get_barrier_semaphore()
    for off in range(1, n_mp):
        pl.semaphore_signal(
            barrier, inc=1, device_id={"dp": dp, "mp": lax.rem(mp + off, n_mp)},
            device_id_type=pl.DeviceIdType.MESH,
        )
    for off in range(1, n_dp):
        pl.semaphore_signal(
            barrier, inc=1, device_id={"dp": lax.rem(dp + off, n_dp), "mp": mp},
            device_id_type=pl.DeviceIdType.MESH,
        )
    pl.semaphore_wait(barrier, n_mp + n_dp - 2)

    half = task_ref.shape[1]
    row = layer_ref[pl.ds(layer_at[0], 1), :].astype(BF16)
    row = jnp.broadcast_to(row.astype(F32), (tasks, row.shape[1])).astype(BF16)
    unit = matmul(task_ref[...].astype(BF16), hyper_ref[:half, :]) + matmul(row, hyper_ref[half:, :])
    unit = jnp.maximum(unit, 0.0)
    hid[mp] = jnp.concatenate([unit, unit], axis=0).astype(BF16)

    def hid_copy(off, block, to):
        return remote(hid.at[block], hid.at[block], hid_s.at[off - 1], hid_r.at[off - 1], to_mp=to)

    def rows_of(step):
        return pl.ds(pl.multiple_of(step * rows, rows), rows)

    def ag_copy(off, step):
        return remote(
            tok.at[rows_of(step)], x_all.at[mp, rows_of(step)],
            ag_s.at[off - 1, step], ag_r.at[off - 1, step], to_mp=far(off) * 2 + core,
        )

    def ag_in(off, step):
        block = x_all.at[src_chip(off) * 2 + core, rows_of(step)]
        return remote(block, block, ag_s.at[off - 1, step], ag_r.at[off - 1, step], to_mp=mate)

    def fw_copy(off, step, which):
        block = x_all.at[src_chip(off) * 2 + which, rows_of(step)]
        return remote(block, block, fw_s.at[off - 1, step], fw_r.at[off - 1, step], to_mp=mate)

    for off in range(1, n_mp):
        hid_copy(off, mp, lax.rem(mp + off, n_mp)).start()
    pair = remote(tok, x_all.at[mp], pair_s, pair_r, to_mp=mate)
    for off in range(1, chips):
        ag_copy(off, 0).start()
    pair.start()

    @pl.loop(1, steps)
    def _(step):
        for off in range(1, chips):
            ag_copy(off, step).start()

    for off in range(1, n_mp):
        hid_copy(off, lax.rem(mp + n_mp - off, n_mp), mp * 0 + lax.rem(mp + off, n_mp)).wait_recv()
    wide_cols = g_down.shape[1]
    tile = min(512, wide_cols)
    gen_rows = wide_cols // LANES * tasks
    deep = hid.shape[2]

    def gen_block(which, at):
        return made_all.at[which, pl.ds(pl.multiple_of(at * gen_rows, gen_rows), gen_rows)]

    def gen_copy(which, off, at, to):
        return remote(
            gen_block(which, at), gen_block(which, at),
            gen_s.at[which, off - 1], gen_r.at[which, off - 1], to_dp=to,
        )

    for which, weights in enumerate((gd, gu)):
        loads[which].wait()

        @pl.loop(0, wide_cols // tile)
        def _(i):
            cols = pl.ds(pl.multiple_of(i * tile, tile), tile)
            total = matmul(hid[0], weights[0:deep, cols])
            for block in range(1, n_mp):
                total += matmul(hid[block], weights[block * deep:(block + 1) * deep, cols])
            base = dp * gen_rows + i * (tile // LANES * tasks)
            for j in range(0, tile // LANES, 2):
                two = [total[:tasks, (j + k) * LANES:(j + k + 1) * LANES] for k in range(2)]
                at = pl.ds(pl.multiple_of(base + j * tasks, 2 * tasks), 2 * tasks)
                made_all[which, at, :] = jnp.concatenate(two, axis=0).astype(BF16)

        for off in range(1, n_dp):
            gen_copy(which, off, dp, lax.rem(dp + off, n_dp)).start()

    def forward(step):
        for off in range(1, chips):
            ag_in(off, step).wait_recv()
            fw_copy(off, step, core).start()

    forward(0)
    own_load.wait()
    pair_in = remote(x_all.at[mate], x_all.at[mate], pair_s, pair_r, to_mp=mate)
    pair_in.wait_recv()
    for load in loads[2:]:
        load.wait()

    def pt_copy(step, q):
        return remote(
            part_away.at[step, q], part_got.at[step, q], pt_s.at[step, q], pt_r.at[step, q], to_mp=mate
        )

    def y_copy(step, off):
        return remote(
            y_out.at[step, off - 1], y_got.at[step, off - 1],
            y_s.at[step, off - 1], y_r.at[step, off - 1], to_mp=far(off) * 2 + core,
        )

    sub = min(64, rows)
    units = wg.shape[1]
    ff_tile = 256 if units % 256 == 0 else units

    @pl.loop(0, steps)
    def _(step):
        for off in range(1, chips):
            fw_copy(off, step, 1 - core).wait_recv()
        gain = gain_ref[...].astype(F32)
        for r in range(0, rows, sub):
            at = pl.ds(pl.multiple_of(step * rows + r, sub), sub)
            wide = jnp.concatenate([x_all[b, at, :] for b in range(n_mp)], axis=1).astype(F32)
            mean = jnp.sum(wide * wide, axis=-1, keepdims=True) * (1.0 / model)
            normed[r:r + sub, :] = (wide * lax.rsqrt(mean + 1e-06) * gain).astype(BF16)
        for f in range(0, units, ff_tile):
            gate = matmul(normed[...], wg[:, f:f + ff_tile])
            linear = matmul(normed[...], wl[:, f:f + ff_tile])
            inner = 0.7978845608028654 * (gate + 0.044715 * (gate * gate * gate))
            act[:, f:f + ff_tile] = (0.5 * gate * (1.0 + jnp.tanh(inner)) * linear).astype(BF16)
        for q in range(chips):
            cols = pl.ds(pl.multiple_of((2 * q + 1 - core) * feat, feat), feat)
            part_away[step, q] = matmul(act[...], wo[:, cols]).astype(BF16)
            pt_copy(step, q).start()
        for q in range(chips):
            cols = pl.ds(pl.multiple_of((2 * q + core) * feat, feat), feat)
            part_mine[step, q] = matmul(act[...], wo[:, cols]).astype(BF16)

        @pl.when(step + 1 < steps)
        def _():
            forward(step + 1)

        for q in range(chips):
            pt_copy(step, q).wait_recv()
        for off in range(1, chips):
            q = far(off)
            y_out[step, off - 1] = (
                part_mine[step, q].astype(F32) + part_got[step, q].astype(F32)
            ).astype(BF16)
            y_copy(step, off).start()

    for which in range(2):
        for off in range(1, n_dp):
            gen_copy(which, off, lax.rem(dp + n_dp - off, n_dp), lax.rem(dp + off, n_dp)).wait_recv()
    fold = LANES // rank
    take = LANES // tasks
    span = take * fold
    r_at = lax.broadcasted_iota(jnp.int32, (tasks * span, LANES), 0)
    c_at = lax.broadcasted_iota(jnp.int32, (tasks * span, LANES), 1)
    f_at, t_at = lax.rem(r_at, span), lax.div(r_at, span)
    pick = (lax.div(c_at, tasks) == lax.div(f_at, fold)) & (lax.rem(c_at, tasks) == t_at)
    pick = jnp.where(pick, 1.0, 0.0).astype(BF16)
    keep = lax.div(c_at, rank) == lax.rem(f_at, fold)
    for which, dst in enumerate((down, up)):

        @pl.loop(0, feat // span)
        def _(b):
            block = made_all[which, pl.ds(pl.multiple_of(b * LANES, LANES), LANES), :]
            spread = jnp.where(keep, matmul(pick, block), 0.0).astype(BF16)
            for t in range(tasks):
                dst[t, pl.ds(pl.multiple_of(b * span, span), span), :] = spread[t * span:(t + 1) * span, :]

    lane = lax.broadcasted_iota(jnp.int32, (seq, LANES), 1)
    low = lane < rank
    per = rows // seq

    def sp_copy(step):
        return remote(sq_mine.at[step], sq_got.at[step], sp_s.at[step], sp_r.at[step], to_mp=mate)

    def sf_copy(step, off):
        return remote(
            sq_chip.at[step], sq_far.at[step, off - 1],
            sf_s.at[step, off - 1], sf_r.at[step, off - 1], to_mp=far(off) * 2 + core,
        )

    @pl.loop(0, steps)
    def _(step):
        for off in range(1, chips):
            y_copy(step, off).wait_recv()
        total = part_mine[step, chip].astype(F32) + part_got[step, chip].astype(F32)
        for off in range(1, chips):
            total += y_got[step, off - 1].astype(F32)
        ff_all[rows_of(step), :] = total.astype(BF16)
        both = []
        for s in range(per):
            at = pl.ds(pl.multiple_of(step * rows + s * seq, seq), seq)
            value = matmul(ff_all[at, :], down[ids_ref[step * per + s]])
            both.append(value + pltpu.roll(value, rank, 1))
        sq_mine[step] = jnp.where(low, both[0], both[1]).astype(BF16)
        sp_copy(step).start()
        sp_copy(step).wait_recv()
        sq_chip[step] = (sq_mine[step].astype(F32) + sq_got[step].astype(F32)).astype(BF16)
        for off in range(1, chips):
            sf_copy(step, off).start()

    def out_copy(step):
        return pltpu.make_async_copy(
            result.at[rows_of(step)], out.at[rows_of(step)], out_sem.at[step]
        )

    @pl.loop(0, steps)
    def _(step):
        for off in range(1, chips):
            sf_copy(step, off).wait_recv()
        total = sq_chip[step].astype(F32)
        for off in range(1, chips):
            total += sq_far[step, off - 1].astype(F32)
        total = jnp.maximum(total, 0.0)
        for s in range(per):
            at = pl.ds(pl.multiple_of(step * rows + s * seq, seq), seq)
            mine = jnp.where(low if s == 0 else jnp.logical_not(low), total, 0.0)
            mine = (mine + pltpu.roll(mine, rank, 1)).astype(BF16)
            expand = lax.dot_general(
                mine, up[ids_ref[step * per + s]], (((1,), (1,)), ((), ())), preferred_element_type=F32
            )
            mixed = x_all[mp, at, :].astype(F32) + ff_all[at, :].astype(F32) + expand
            result[at, :] = mixed.astype(BF16)
        out_copy(step).start()

    pair.wait_send()
    for off in range(1, n_mp):
        hid_copy(off, mp, lax.rem(mp + off, n_mp)).wait_send()
    for which in range(2):
        for off in range(1, n_dp):
            gen_copy(which, off, dp, lax.rem(dp + off, n_dp)).wait_send()

    @pl.loop(0, steps)
    def _(step):
        for off in range(1, chips):
            ag_copy(off, step).wait_send()
            fw_copy(off, step, core).wait_send()
            y_copy(step, off).wait_send()
            sf_copy(step, off).wait_send()
        for q in range(chips):
            pt_copy(step, q).wait_send()
        sp_copy(step).wait_send()
        out_copy(step).wait()


def per_device(
    n_dp, n_mp,
    tokens, norm_gain, wi_gate, wi_linear, wo_out, task_table, layer_table,
    task_ids, layer_index, hyper_in, gen_down, gen_up,
):
    rows_all, feat = tokens.shape
    seqs = task_ids.shape[0]
    seq = rows_all // seqs
    rank = gen_down.shape[1] * n_dp // feat
    per = LANES // rank
    rows = seq * per
    steps = rows_all // rows
    chips = n_mp // 2
    tasks = task_table.shape[0]
    model = feat * n_mp
    dma = pltpu.SemaphoreType.DMA
    vmem = pltpu.VMEM
    far = chips - 1
    gen_rows = feat * rank // LANES * tasks
    smem = pl.BlockSpec(memory_space=pltpu.SMEM)
    inside = pl.BlockSpec(memory_space=pltpu.VMEM)
    hbm = pl.BlockSpec(memory_space=pl.ANY)
    flops = 2 * rows_all * model * wi_gate.shape[1] * 3
    return pl.pallas_call(
        functools.partial(kernel, n_dp, n_mp, rank),
        name="adapter_ffn",
        out_shape=jax.ShapeDtypeStruct(tokens.shape, BF16),
        in_specs=[smem, smem, inside, inside, inside, inside] + [hbm] * 6,
        out_specs=hbm,
        scratch_shapes=[
            vmem((n_mp, rows_all, feat), BF16),
            vmem(wi_gate.shape, BF16),
            vmem(wi_linear.shape, BF16),
            vmem(wo_out.shape, BF16),
            vmem(gen_down.shape, BF16),
            vmem(gen_up.shape, BF16),
            vmem((rows, model), BF16),
            vmem((rows, wi_gate.shape[1]), BF16),
            vmem((n_mp, 2 * tasks, hyper_in.shape[1]), BF16),
            vmem((2, gen_rows, LANES), BF16),
            vmem((tasks, feat, LANES), BF16),
            vmem((tasks, feat, LANES), BF16),
            vmem((steps, chips, rows, feat), BF16),
            vmem((steps, chips, rows, feat), BF16),
            vmem((steps, chips, rows, feat), BF16),
            vmem((steps, far, rows, feat), BF16),
            vmem((steps, far, rows, feat), BF16),
            vmem((rows_all, feat), BF16),
            vmem((steps, seq, LANES), BF16),
            vmem((steps, seq, LANES), BF16),
            vmem((steps, seq, LANES), BF16),
            vmem((steps, far, seq, LANES), BF16),
            vmem((rows_all, feat), BF16),
            dma((6,)),
            dma((steps,)),
            dma((far, steps)), dma((far, steps)),
            dma, dma,
            dma((far, steps)), dma((far, steps)),
            dma((n_mp - 1,)), dma((n_mp - 1,)),
            dma((2, n_dp - 1)), dma((2, n_dp - 1)),
            dma((steps, chips)), dma((steps, chips)),
            dma((steps, far)), dma((steps, far)),
            dma((steps,)), dma((steps,)),
            dma((steps, far)), dma((steps, far)),
        ],
        compiler_params=pltpu.CompilerParams(
            collective_id=0, has_side_effects=True, vmem_limit_bytes=62 * 1024 * 1024
        ),
        cost_estimate=pl.CostEstimate(flops=flops, bytes_accessed=34_000_000, transcendentals=0),
    )(
        task_ids, layer_index, norm_gain.reshape(1, -1), task_table, layer_table, hyper_in,
        tokens, wi_gate, wi_linear, wo_out, gen_down, gen_up,
    )


def solution(mesh):
    return jax.shard_map(
        functools.partial(per_device, mesh.shape["dp"], mesh.shape["mp"]),
        mesh=mesh,
        in_specs=(
            P("dp", "mp"),
            P(),
            P(None, "mp"),
            P(None, "mp"),
            P("mp", None),
            P(),
            P(),
            P("dp"),
            P(),
            P(None, "mp"),
            P(None, ("mp", "dp")),
            P(None, ("mp", "dp")),
        ),
        out_specs=P("dp", "mp"),
        check_vma=False,
    )
```
